32 devices in a mesh: groups: 2 (over x), seq: 16 (over z, y, core).
Axes of the slice: x: 2, y: 2, z: 4, core: 2. Of those that a mesh axis runs over, the one named last changes fastest.
Arguments:
- mixed_input: bfloat16 [8192, 2816], P(('groups', 'seq')), parts along dimension 0, may hold values from -6 to 6
- step_raw: float32 [40, 8192], P(None, ('groups', 'seq')), parts along dimension 1, may hold values from -2.5 to 5.5
- conv_weight: float32 [4, 2816], replicated, may hold values from -1.5 to 1.5
- conv_bias: float32 [2816], replicated, may hold values from -1.2 to 1.2
- step_bias: float32 [40], replicated, may hold values from -5 to -3
- decay_log: float32 [40], replicated, may hold values from -12 to 1
- skip_gain: float32 [40], replicated, may hold values from 0.5 to 1.5
- result_cotangent: bfloat16 [8192, 2560], P(('groups', 'seq')), parts along dimension 0, may hold values from -1.1953125 to 1.1953125
- entry_state: float32 [32, 40, 64, 128], P(('groups', 'seq')), parts along dimension 0, may hold values from -3 to 3
Outputs:
- input_grad: float32 [8192, 2816], P(('groups', 'seq')), parts along dimension 0
- step_grad: float32 [40, 8192], P(None, ('groups', 'seq')), parts along dimension 1
- kernel_grad: float32 [8, 2816], P('groups'), parts along dimension 0
- offset_grad: float32 [5632], P('groups'), parts along dimension 0
- bias_grad: float32 [80], P('groups'), parts along dimension 0
- decay_grad: float32 [80], P('groups'), parts along dimension 0
- skip_grad: float32 [80], P('groups'), parts along dimension 0
The draws below stay inside these ranges and needn't reach their ends.
There are 2 independent parts, one for each index of `groups`. The reference program is written for one: setup_inputs(seed, part) draws one part's arguments, and reference() takes and returns one part's arrays. A program takes and returns all parts, laid end to end along the dimension named above; an argument that names none is the same for every part. Nothing has to cross between parts.
All inputs are finite; a program needn't handle non-finite values.
Results may differ from the reference program's by a relative error of at most 0.0003.
Values may be sent and summed in bfloat16 or wider, within the bound.
A program may use at most 384 MiB of HBM per device.

```python
import jax
import jax.numpy as jnp
from jax import lax

HEADS = 40
HEAD_DIM = 64
STATE = 128
CONV_W = 4
BLOCK = 256
TOK_DEV = 256
TIMELINE_EXTENT = 4096
INNER = 2560
CHANNELS = 2816
N_SEQ = 16


def draw_step_raw(key, part):
    first, second, third = jax.random.split(key, 3)
    starting_index = jnp.clip(0.6 * jax.random.normal(first, (HEADS, TIMELINE_EXTENT), jnp.float32), -1.8, 1.8)
    shards = TIMELINE_EXTENT // TOK_DEV
    index_displacement = jax.random.uniform(second, (1, shards), jnp.float32, -0.7, 0.7)
    index_displacement = jnp.repeat(index_displacement, TOK_DEV, axis=1)
    accelerator_slots = jax.random.randint(third, (4,), 0, TIMELINE_EXTENT)
    element_window = jnp.any(jnp.arange(TIMELINE_EXTENT)[None, :] == accelerator_slots[:, None], axis=0)
    return (starting_index + index_displacement + 3.0 * element_window.astype(jnp.float32)[None, :]).astype(jnp.float32)


def draw_decay_log(key, part):
    first, second = jax.random.split(key, 2)
    share = 0.5
    quick = jax.random.uniform(first, (HEADS,), jnp.float32) < share
    spread = jax.random.uniform(second, (HEADS,), jnp.float32)
    quick_log = spread * jnp.log(2.5)
    slow_log = jnp.log(0.2 / (0.018 * TIMELINE_EXTENT)) + spread * jnp.log(5.0)
    return jnp.where(quick, quick_log, slow_log).astype(jnp.float32)


def block_levels(own_key, extent, cuts, smallest, largest):
    gain = 1.0
    for dim, shards_of in cuts:
        draws = jax.random.uniform(jax.random.fold_in(jax.random.fold_in(own_key, 6), dim), (shards_of,), jnp.float32, smallest / len(cuts), largest / len(cuts))
        gain = gain * jnp.repeat(jnp.exp(draws), extent[dim] // shards_of).reshape((-1,) + (1,) * (len(extent) - 1 - dim))
    return gain


def scatter_about(key, extent, scale, most, cuts=(), held_as=jnp.bfloat16):
    array = jax.random.normal(key, extent, jnp.float32) * scale
    if len(cuts) > 0:
        array = block_levels(key, extent, cuts, -0.22, 0.18) * array
    return jnp.clip(array, min=-most, max=most).astype(held_as)


def setup_inputs(seed: int = 0, part: int = 0) -> dict:
    streams_of = jax.random.split(jax.random.key(seed), 10)
    part_keys = jax.random.split(jax.random.fold_in(streams_of[9], part), 10)
    mixed_input = scatter_about(part_keys[0], (TIMELINE_EXTENT, CHANNELS), 1.0, 6.0, ((0, 16),))
    step_raw = draw_step_raw(jax.random.fold_in(jax.random.fold_in(streams_of[9], part), 71), part)
    conv_weight = scatter_about(streams_of[2], (CONV_W, CHANNELS), 0.25, 1.5, (), jnp.float32)
    conv_bias = scatter_about(streams_of[3], (CHANNELS,), 0.2, 1.2, (), jnp.float32)
    step_bias = jnp.clip(jax.random.uniform(streams_of[4], (HEADS,), jnp.float32, -5.0, -3.0), -5.0, -3.0)
    decay_log = draw_decay_log(jax.random.fold_in(streams_of[9], 71), part)
    skip_gain = jnp.clip(jax.random.uniform(streams_of[6], (HEADS,), jnp.float32, 0.5, 1.5), 0.5, 1.5)
    result_cotangent = scatter_about(part_keys[7], (TIMELINE_EXTENT, INNER), 0.2, 1.1953125, ((0, 16),))
    entry_state = scatter_about(part_keys[8], (N_SEQ, HEADS, HEAD_DIM, STATE), 0.5, 3.0, ((0, 16),), jnp.float32)
    return {"mixed_input": mixed_input, "step_raw": step_raw, "conv_weight": conv_weight, "conv_bias": conv_bias, "step_bias": step_bias, "decay_log": decay_log, "skip_gain": skip_gain, "result_cotangent": result_cotangent, "entry_state": entry_state}


highest = lax.Precision.HIGHEST

def block_terms(signal, writes, reads, steps, decays):
    running = jnp.cumsum(decays, axis=0)
    scaled = signal * steps[:, :, None]
    scores = jnp.dot(reads, writes.T, precision=highest, preferred_element_type=jnp.float32)
    span = running.shape[0]
    causal_mask = lax.broadcasted_iota(jnp.int32, (span, span), 1) <= lax.broadcasted_iota(jnp.int32, (span, span), 0)
    spread = running[:, None, :] - running[None, :, :]
    fading = jnp.exp(jnp.where(causal_mask[:, :, None], spread, -jnp.inf))
    inside = jnp.einsum('tsh,shp->thp', fading * scores[:, :, None], scaled, precision=highest)
    remain = jnp.exp(running[-1][None, :] - running)
    block_state = jnp.einsum('thp,tn->hpn', scaled * remain[:, :, None], writes, precision=highest)
    return (inside, block_state, running)

def front_part(extended, step_raw, conv_weight, conv_bias, step_bias, decay_log):
    tok_rows = extended.shape[0] - conv_weight.shape[0] + 1
    convolved = jnp.zeros((tok_rows, extended.shape[1]), jnp.float32) + conv_bias[None, :]
    for index in range(conv_weight.shape[0]):
        convolved = convolved + conv_weight[index][None, :] * extended[index:index + tok_rows]
    activated = jax.nn.silu(convolved)
    inner_width = HEADS * HEAD_DIM
    signal = activated[:, :inner_width].reshape(tok_rows, HEADS, HEAD_DIM)
    writes = activated[:, inner_width:inner_width + STATE]
    reads = activated[:, inner_width + STATE:]
    steps = jax.nn.softplus(step_raw.T + step_bias[None, :])
    decays = -steps * jnp.exp(decay_log)[None, :]
    return (signal, writes, reads, steps, decays)

def reference(mixed_input, step_raw, conv_weight, conv_bias, step_bias, decay_log, skip_gain, result_cotangent, entry_state):
    per_shard = TOK_DEV // BLOCK

    def forward_pass(extended, step_raw, conv_weight, conv_bias, step_bias, decay_log, skip_gain):
        signal, writes, reads, steps, decays = front_part(extended, step_raw, conv_weight, conv_bias, step_bias, decay_log)
        number = TIMELINE_EXTENT // BLOCK
        pieces = (signal.reshape(number, BLOCK, HEADS, HEAD_DIM), writes.reshape(number, BLOCK, STATE), reads.reshape(number, BLOCK, STATE), steps.reshape(number, BLOCK, HEADS), decays.reshape(number, BLOCK, HEADS), jnp.arange(number, dtype=jnp.int32))

        def advance(handed_along, piece):
            position = piece[5]
            shard = (position // per_shard).astype(jnp.int32)
            saved = lax.dynamic_index_in_dim(entry_state, shard, 0, keepdims=False)
            replaced = saved + handed_along - lax.stop_gradient(handed_along)
            handed_along = jnp.where(position % per_shard == 0, replaced, handed_along)
            inside, block_state, running = block_terms(piece[0], piece[1], piece[2], piece[3], piece[4])
            beyond = jnp.exp(running)[:, :, None] * jnp.einsum('tn,hpn->thp', piece[2], handed_along, precision=highest)
            renewed = jnp.exp(running[-1])[:, None, None] * handed_along + block_state
            return (renewed, inside + beyond)
        initial = jnp.zeros((HEADS, HEAD_DIM, STATE), jnp.float32)
        _, produced_results = lax.scan(jax.checkpoint(advance), initial, pieces)
        return produced_results.reshape(TIMELINE_EXTENT, HEADS, HEAD_DIM) + skip_gain[None, :, None] * signal
    leading = jnp.zeros((CONV_W - 1, CHANNELS), jnp.float32)
    extended = jnp.concatenate([leading, mixed_input.astype(jnp.float32)], 0)
    _, pullback = jax.vjp(forward_pass, extended, step_raw, conv_weight, conv_bias, step_bias, decay_log, skip_gain)
    gradients = pullback(result_cotangent.astype(jnp.float32).reshape(TIMELINE_EXTENT, HEADS, HEAD_DIM))
    return (gradients[0][CONV_W - 1:], gradients[1], gradients[2], gradients[3], gradients[4], gradients[5], gradients[6])
```

```python
import functools

import jax
import jax.numpy as jnp
from jax import lax
from jax.experimental import pallas as pl
from jax.experimental.pallas import tpu as pltpu
from jax.sharding import PartitionSpec as P

F32 = jnp.float32
BF16 = jnp.bfloat16
LANES = 128
WIDE = 256
LOG2E = 1.4426950408889634
MESH = pl.DeviceIdType.MESH


def split2(v):
    hi = v.astype(BF16)
    return hi, (v - hi.astype(F32)).astype(BF16)


def split3(v):
    hi = v.astype(BF16)
    rest = v - hi.astype(F32)
    mid = rest.astype(BF16)
    return hi, mid, (rest - mid.astype(F32)).astype(BF16)


def nn(a, b):
    return lax.dot_general(a, b, (((1,), (0,)), ((), ())), preferred_element_type=F32)


def nt(a, b):
    return lax.dot_general(a, b, (((1,), (1,)), ((), ())), preferred_element_type=F32)


def both(dot, a, b):
    return dot(a[0], b[0]) + dot(a[1], b[0]) + dot(a[0], b[1])


def iota(shape, dim):
    return lax.broadcasted_iota(jnp.int32, shape, dim)


def body(
    n, heads, width,
    xin, raw, conv_w, conv_b, cols, skip, cot, state,
    ig, step_g, kg_out, off_out, small_out,
    ext, x_s, ds_s, run_s, steps_s, p128, run_t, dxs_s, st_hi, st_lo, gt, et, f_s,
    gram, dgram, dpos, acc_c, acc_b, q_acc, r_acc, last_acc, skip_acc, dconv, halo_in, bf_buf, bf_in,
    send_sem, recv_sem, halo_sem, back_sem, sum_sem,
):
    tok = xin.shape[0]
    chan = xin.shape[1]
    inner = heads * width
    pairs = inner // LANES
    quads = inner // WIDE
    idx = lax.axis_index("seq")
    rounds = n.bit_length() - 1
    has_prev, has_next = idx > 0, idx < n - 1

    def to(where):
        return {"seq": where}

    barrier = pltpu.get_barrier_semaphore()

    @pl.when(has_prev)
    def _():
        pl.semaphore_signal(barrier, inc=1, device_id=to(idx - 1), device_id_type=MESH)

    @pl.when(has_next)
    def _():
        pl.semaphore_signal(barrier, inc=1, device_id=to(idx + 1), device_id_type=MESH)

    def partner(k):
        bit = 1 << k
        return jnp.where((idx // bit) % 2 == 0, idx + bit, idx - bit)

    for k in range(1, rounds):
        pl.semaphore_signal(barrier, inc=1, device_id=to(partner(k)), device_id_type=MESH)
    pl.semaphore_wait(barrier, rounds - 1 + has_prev.astype(jnp.int32) + has_next.astype(jnp.int32))

    halo_copy = pltpu.make_async_remote_copy(
        src_ref=xin.at[pl.ds(tok - 16, 16)], dst_ref=halo_in,
        send_sem=halo_sem.at[0], recv_sem=halo_sem.at[1],
        device_id=to(idx + 1), device_id_type=MESH,
    )

    @pl.when(has_next)
    def _():
        halo_copy.start()

    z = raw[...] + cols[:, 0:1]
    steps_t = jnp.maximum(z, 0.0) + jnp.log1p(jnp.exp(-jnp.abs(z)))
    rate = jnp.exp(cols[:, 1:2])
    p128[...] = jnp.zeros_like(p128)
    p128[0:heads, :] = -steps_t * rate * LOG2E
    upper = jnp.where(iota((tok, tok), 0) <= iota((tok, tok), 1), 1.0, 0.0).astype(BF16)
    lower = jnp.where(iota((tok, tok), 0) >= iota((tok, tok), 1), 1.0, 0.0).astype(BF16)
    parts = split3(p128[...])
    run_rows = nn(parts[0], upper) + nn(parts[1], upper) + nn(parts[2], upper)
    run_t[...] = run_rows
    run_col = split3(run_rows.T)
    p128[0:heads, :] = steps_t
    steps_col = p128[...].T
    steps_parts = split3(steps_col)

    def onehot(quad):
        return jnp.where(
            iota((LANES, WIDE), 0) == iota((LANES, WIDE), 1) // width + quad * (WIDE // width), 1.0, 0.0
        ).astype(BF16)

    def onehot_t(quad):
        return jnp.where(
            iota((WIDE, LANES), 1) == iota((WIDE, LANES), 0) // width + quad * (WIDE // width), 1.0, 0.0
        ).astype(BF16)

    @pl.loop(0, quads)
    def _(q):
        at = pl.ds(pl.multiple_of(q * WIDE, WIDE), WIDE)
        pick = onehot(q)
        run = nn(run_col[0], pick) + nn(run_col[1], pick) + nn(run_col[2], pick)
        run_s[:, at] = run
        steps_s[:, at] = nn(steps_parts[0], pick) + nn(steps_parts[1], pick) + nn(steps_parts[2], pick)
        fade = jnp.exp2(run[tok - 1 : tok])
        f_s[2 * q] = jnp.broadcast_to(fade[:, :LANES], (8, LANES))
        f_s[2 * q + 1] = jnp.broadcast_to(fade[:, LANES:], (8, LANES))

    @pl.when(has_prev)
    def _():
        halo_copy.wait_recv()
        ext[0:8] = halo_in[8:16].astype(F32)

    @pl.when(jnp.logical_not(has_prev))
    def _():
        ext[0:8] = jnp.zeros((8, chan), F32)

    def front(q):
        at = pl.ds(pl.multiple_of(q * WIDE, WIDE), WIDE)
        ext[8 : tok + 8, at] = xin[:, at].astype(F32)
        value = jnp.broadcast_to(conv_b[:, at], (tok, WIDE))
        for k in range(4):
            value = value + conv_w[k : k + 1, at] * ext[5 + k : 5 + k + tok, at]
        gate = 1.0 / (1.0 + jnp.exp(-value))
        x_s[:, at] = value * gate
        ds_s[:, at] = gate * (1.0 + value * (1.0 - gate))

    front(quads)
    writes = x_s[:, inner : inner + LANES]
    reads = x_s[:, inner + LANES :]
    b2 = split2(writes)
    c2 = split2(reads)
    ct2 = split2(reads.T)

    @pl.loop(0, quads)
    def _(q):
        at = pl.ds(pl.multiple_of(q * WIDE, WIDE), WIDE)
        w = split2(jnp.exp2(run_s[:, at]) * cot[:, at].astype(F32))
        g = both(nn, ct2, w)
        gt[2 * q] = g[:, :LANES]
        gt[2 * q + 1] = g[:, LANES:]

    def chunk(p):
        return pltpu.make_async_remote_copy(
            src_ref=gt.at[p], dst_ref=et.at[p],
            send_sem=send_sem.at[p], recv_sem=recv_sem.at[p],
            device_id=to(idx - 1), device_id_type=MESH,
        )

    def chain():
        @pl.loop(0, pairs)
        def _(p):
            @pl.when(has_next)
            def _():
                chunk(p).wait_recv()
                gt[p] = gt[p] + f_s[p][0:1] * et[p]

            @pl.when(jnp.logical_not(has_next))
            def _():
                et[p] = jnp.zeros((LANES, LANES), F32)

            @pl.when(has_prev)
            def _():
                chunk(p).start()

    early = idx >= n // 2

    @pl.when(early)
    def _():
        chain()

    gram[...] = both(nt, b2, c2)
    dgram[...] = jnp.zeros_like(dgram)
    acc_c[...] = jnp.zeros_like(acc_c)
    acc_b[...] = jnp.zeros_like(acc_b)
    q_acc[...] = jnp.zeros_like(q_acc)
    r_acc[...] = jnp.zeros_like(r_acc)
    last_acc[...] = jnp.zeros_like(last_acc)
    skip_acc[...] = jnp.zeros_like(skip_acc)
    dpos[...] = jnp.zeros_like(dpos)

    @pl.loop(0, quads)
    def _(q):
        at = pl.ds(pl.multiple_of(q * WIDE, WIDE), WIDE)
        front(q)
        dy = cot[:, at].astype(F32)
        w = jnp.exp2(run_s[:, at]) * dy
        st = state[at, :].T
        hi, lo = split2(st)
        st_hi[:, at] = hi
        st_lo[:, at] = lo
        acc_c[...] += both(nt, split2(w), (hi, lo))
        zy = split2(both(nn, c2, (hi, lo)) * w)
        pick = onehot_t(q)
        r_acc[...] += nn(zy[0], pick) + nn(zy[1], pick)
        sk = split2(jnp.broadcast_to(jnp.sum(dy * x_s[:, at], axis=0, keepdims=True), (8, WIDE)))
        skip_acc[...] += nn(sk[0], pick) + nn(sk[1], pick)

    low = iota((tok, LANES), 1) < width
    mask = iota((tok, tok), 0) <= iota((tok, tok), 1)

    @pl.loop(0, pairs)
    def _(p):
        at = pl.ds(pl.multiple_of(p * LANES, LANES), LANES)
        dy = cot[:, at]
        dy_f = dy.astype(F32)
        xs = x_s[:, at] * steps_s[:, at]
        run = run_s[:, at]
        turned = pltpu.roll(run, width, 1)
        twice = jnp.concatenate([dy, dy], axis=1)
        total = jnp.zeros((tok, LANES), F32)
        for half in range(2):
            mine = low if half == 0 else jnp.logical_not(low)
            x_hi, x_lo = split2(jnp.where(mine, xs, 0.0))
            dm = nt(jnp.concatenate([x_hi, x_lo], axis=1), twice)
            own = jnp.where(mine, run, turned)
            own = jnp.concatenate([own, own], axis=1)
            gap = run_t[pl.ds(2 * p + half, 1), :] - own
            fade = jnp.exp2(jnp.where(mask, gap, -jnp.inf))
            ldm = fade * dm
            dgram[...] += ldm
            m = fade * gram[...]
            dpos[pl.ds(2 * p + half, 1), :] = jnp.sum(m * dm, axis=0, keepdims=True)
            m_hi, m_lo = split2(m)
            dy_m = jnp.where(mine, dy_f, 0.0).astype(BF16)
            total = total + nn(m_hi, dy_m) + nn(m_lo, dy_m)
        dxs_s[:, at] = total

    @pl.when(jnp.logical_not(early))
    def _():
        chain()

    @pl.loop(0, quads)
    def _(q):
        at = pl.ds(pl.multiple_of(q * WIDE, WIDE), WIDE)
        e = jnp.concatenate([et[2 * q], et[2 * q + 1]], axis=1)
        e2 = split2(e)
        run = run_s[:, at]
        remain = jnp.exp2(run[tok - 1 : tok] - run)
        rv = remain * both(nn, b2, e2)
        steps = steps_s[:, at]
        x = x_s[:, at]
        dxs = rv + dxs_s[:, at]
        xs = x * steps
        pick = onehot_t(q)
        part = split2(x * dxs)
        q_acc[...] += nn(part[0], pick) + nn(part[1], pick)
        st = st_hi[:, at].astype(F32) + st_lo[:, at].astype(F32)
        fade = jnp.exp2(run[tok - 1 : tok])
        end = jnp.sum(xs * rv, axis=0, keepdims=True) + fade * jnp.sum(e * st, axis=0, keepdims=True)
        end = split3(jnp.broadcast_to(end, (8, WIDE)))
        last_acc[...] += nn(end[0], pick) + nn(end[1], pick) + nn(end[2], pick)
        acc_b[...] += both(nt, split2(xs * remain), e2)
        lane = iota((1, WIDE), 1) // width
        gain = jnp.zeros((1, WIDE), F32)
        for j in range(WIDE // width):
            gain = jnp.where(lane == j, skip[q * (WIDE // width) + j], gain)
        dx = dxs * steps + gain * cot[:, at].astype(F32)
        dconv[0:tok, at] = dx * ds_s[:, at]

    dg = split2(dgram[...])
    dgt = split2(dgram[...].T)
    tail = pl.ds(inner, LANES)
    dconv[0:tok, tail] = (acc_b[...] + both(nn, dg, c2)) * ds_s[:, tail]
    tail = pl.ds(inner + LANES, LANES)
    dconv[0:tok, tail] = (acc_c[...] + both(nn, dgt, b2)) * ds_s[:, tail]

    back = pltpu.make_async_remote_copy(
        src_ref=dconv.at[pl.ds(0, 8)], dst_ref=dconv.at[pl.ds(tok, 8)],
        send_sem=back_sem.at[0], recv_sem=back_sem.at[1],
        device_id=to(idx - 1), device_id_type=MESH,
    )

    @pl.when(has_prev)
    def _():
        back.start()

    @pl.when(jnp.logical_not(has_next))
    def _():
        dconv[tok : tok + 8] = jnp.zeros((8, chan), F32)

    drun = r_acc[...] - steps_col * q_acc[...]
    drun = drun + jnp.where(iota((tok, LANES), 0) == tok - 1, last_acc[0:1, :], 0.0)
    dp = split3(drun.T + dpos[...])
    ddecay = (nn(dp[0], lower) + nn(dp[1], lower) + nn(dp[2], lower))[0:heads]
    dsteps = q_acc[...].T[0:heads] - ddecay * rate
    sg = dsteps / (1.0 + jnp.exp(-z))
    step_g[...] = sg
    p128[0:heads, :] = sg
    bf_buf[0, 5:6, 0:LANES] = jnp.sum(p128[...].T, axis=0, keepdims=True)
    p128[0:heads, :] = -ddecay * steps_t * rate
    bf_buf[0, 5:6, LANES : 2 * LANES] = jnp.sum(p128[...].T, axis=0, keepdims=True)
    bf_buf[0, 5:6, 2 * LANES : 3 * LANES] = skip_acc[0:1]
    bf_buf[0, 5:6, 3 * LANES :] = jnp.zeros((1, chan - 3 * LANES), F32)
    bf_buf[0, 6:8, :] = jnp.zeros((2, chan), F32)

    @pl.loop(0, chan // LANES)
    def _(q):
        at = pl.ds(pl.multiple_of(q * LANES, LANES), LANES)
        d = dconv[0:tok, at]
        for k in range(4):
            bf_buf[0, k : k + 1, at] = jnp.sum(d * ext[5 + k : 5 + k + tok, at], axis=0, keepdims=True)
        bf_buf[0, 4:5, at] = jnp.sum(d, axis=0, keepdims=True)

    def swap(k):
        return pltpu.make_async_remote_copy(
            src_ref=bf_buf.at[k], dst_ref=bf_in.at[k],
            send_sem=sum_sem.at[k], recv_sem=sum_sem.at[rounds + k],
            device_id=to(partner(k)), device_id_type=MESH,
        )

    swap(0).start()

    @pl.when(has_next)
    def _():
        back.wait_recv()

    @pl.loop(0, chan // LANES)
    def _(q):
        at = pl.ds(pl.multiple_of(q * LANES, LANES), LANES)
        value = conv_w[3:4, at] * dconv[0:tok, at]
        for k in range(3):
            value = value + conv_w[k : k + 1, at] * dconv[3 - k : 3 - k + tok, at]
        ig[:, at] = value

    for k in range(rounds):
        swap(k).wait_recv()
        bf_buf[k + 1] = bf_buf[k] + bf_in[k]
        if k + 1 < rounds:
            swap(k + 1).start()
    kg_out[...] = bf_buf[rounds, 0:4]
    off_out[...] = bf_buf[rounds, 4:5]
    for j in range(3):
        small_out[j : j + 1, :] = bf_buf[rounds, 5:6, j * LANES : (j + 1) * LANES]

    for k in range(rounds):
        swap(k).wait_send()

    @pl.when(has_next)
    def _():
        halo_copy.wait_send()

    @pl.when(has_prev)
    def _():
        back.wait_send()

        @pl.loop(0, pairs)
        def _(p):
            chunk(p).wait_send()


def per_device(
    mixed_input, step_raw, conv_weight, conv_bias, step_bias, decay_log, skip_gain, result_cotangent, entry_state
):
    tok, chan = mixed_input.shape
    _, heads, width, span = entry_state.shape
    inner = heads * width
    n = lax.axis_size("seq")
    rounds = n.bit_length() - 1
    pairs = inner // LANES
    cols = jnp.stack([step_bias, decay_log], axis=1)
    vmem = pl.BlockSpec(memory_space=pltpu.VMEM)
    scr = lambda *shape: pltpu.VMEM(shape, F32)
    outs = pl.pallas_call(
        functools.partial(body, n, heads, width),
        out_shape=(
            jax.ShapeDtypeStruct((tok, chan), F32),
            jax.ShapeDtypeStruct((heads, tok), F32),
            jax.ShapeDtypeStruct((4, chan), F32),
            jax.ShapeDtypeStruct((1, chan), F32),
            jax.ShapeDtypeStruct((3, LANES), F32),
        ),
        in_specs=[vmem] * 5 + [pl.BlockSpec(memory_space=pltpu.SMEM)] + [vmem] * 2,
        out_specs=(vmem,) * 5,
        scratch_shapes=[
            scr(tok + 8, chan),
            scr(tok, chan),
            scr(tok, chan),
            scr(tok, inner),
            scr(tok, inner),
            scr(LANES, tok),
            scr(LANES, tok),
            scr(tok, inner),
            pltpu.VMEM((span, inner), BF16),
            pltpu.VMEM((span, inner), BF16),
            scr(pairs, span, LANES),
            scr(pairs, span, LANES),
            scr(pairs, 8, LANES),
            scr(tok, tok),
            scr(tok, tok),
            scr(LANES, tok),
            scr(tok, LANES),
            scr(tok, LANES),
            scr(tok, LANES),
            scr(tok, LANES),
            scr(8, LANES),
            scr(8, LANES),
            scr(tok + 8, chan),
            pltpu.VMEM((16, chan), BF16),
            scr(rounds + 1, 8, chan),
            scr(rounds, 8, chan),
            pltpu.SemaphoreType.DMA((pairs,)),
            pltpu.SemaphoreType.DMA((pairs,)),
            pltpu.SemaphoreType.DMA((2,)),
            pltpu.SemaphoreType.DMA((2,)),
            pltpu.SemaphoreType.DMA((2 * rounds,)),
        ],
        compiler_params=pltpu.CompilerParams(
            collective_id=0, has_side_effects=True, vmem_limit_bytes=60 * 1024 * 1024
        ),
    )(
        mixed_input, step_raw, conv_weight, conv_bias.reshape(1, chan), cols, skip_gain,
        result_cotangent, entry_state.reshape(inner, span),
    )
    grad, step_g, kg, off, small = outs
    return (grad, step_g, kg, off[0], small[0, :heads], small[1, :heads], small[2, :heads])


def solution(mesh):
    rows = ("groups", "seq")
    return jax.shard_map(
        per_device,
        mesh=mesh,
        in_specs=(
            P(rows, None), P(None, rows), P(), P(), P(), P(), P(), P(rows, None), P(rows, None, None, None),
        ),
        out_specs=(P(rows, None), P(None, rows), P("groups", None), P("groups"), P("groups"), P("groups"), P("groups")),
        check_vma=False,
    )
```

```python
import functools

import jax
import jax.numpy as jnp
from jax import lax
from jax.experimental import pallas as pl
from jax.experimental.pallas import tpu as pltpu
from jax.sharding import PartitionSpec as P

F32 = jnp.float32
BF16 = jnp.bfloat16
LANES = 128
WIDE = 256
LOG2E = 1.4426950408889634
MESH = pl.DeviceIdType.MESH


def split2(v):
    hi = v.astype(BF16)
    return hi, (v - hi.astype(F32)).astype(BF16)


def split3(v):
    hi = v.astype(BF16)
    rest = v - hi.astype(F32)
    mid = rest.astype(BF16)
    return hi, mid, (rest - mid.astype(F32)).astype(BF16)


def nn(a, b):
    return lax.dot_general(a, b, (((1,), (0,)), ((), ())), preferred_element_type=F32)


def nt(a, b):
    return lax.dot_general(a, b, (((1,), (1,)), ((), ())), preferred_element_type=F32)


def both(dot, a, b):
    return dot(a[0], b[0]) + dot(a[1], b[0]) + dot(a[0], b[1])


def iota(shape, dim):
    return lax.broadcasted_iota(jnp.int32, shape, dim)


def body(
    n, heads, width,
    xin, raw, conv_w, conv_b1, bias, decay, skip, cot, state,
    ig, step_g, sums_out,
    ext, x_s, ds_s, run_s, steps_s, p128, run_t, dxs_s, st_hi, st_lo, gt, et, f_s,
    gram, dgram, dpos, acc_c, acc_b, q_acc, r_acc, last_acc, skip_acc, dconv, conv_b, z_s, rate_s, halo_in, bf_buf, bf_in,
    send_sem, recv_sem, halo_sem, back_sem, sum_sem,
):
    tok = xin.shape[0]
    chan = xin.shape[1]
    inner = heads * width
    pairs = inner // LANES
    quads = inner // WIDE
    idx = lax.axis_index("seq")
    rounds = n.bit_length() - 1
    has_prev, has_next = idx > 0, idx < n - 1

    def to(where):
        return {"seq": where}

    barrier = pltpu.get_barrier_semaphore()

    @pl.when(has_prev)
    def _():
        pl.semaphore_signal(barrier, inc=1, device_id=to(idx - 1), device_id_type=MESH)

    @pl.when(has_next)
    def _():
        pl.semaphore_signal(barrier, inc=1, device_id=to(idx + 1), device_id_type=MESH)

    def partner(k):
        bit = 1 << k
        return jnp.where((idx // bit) % 2 == 0, idx + bit, idx - bit)

    for k in range(1, rounds):
        pl.semaphore_signal(barrier, inc=1, device_id=to(partner(k)), device_id_type=MESH)
    pl.semaphore_wait(barrier, rounds - 1 + has_prev.astype(jnp.int32) + has_next.astype(jnp.int32))

    halo_copy = pltpu.make_async_remote_copy(
        src_ref=xin.at[pl.ds(tok - 16, 16)], dst_ref=halo_in,
        send_sem=halo_sem.at[0], recv_sem=halo_sem.at[1],
        device_id=to(idx + 1), device_id_type=MESH,
    )

    @pl.when(has_next)
    def _():
        halo_copy.start()

    conv_b[...] = conv_b1[...].reshape(1, chan)

    @pl.loop(0, heads)
    def _(h):
        at = pl.ds(h, 1)
        z_s[at] = raw[at] + bias[h]
        rate_s[at] = jnp.exp(jnp.full((1, tok), decay[h], F32))

    z = z_s[...]
    steps_t = jnp.maximum(z, 0.0) + jnp.log1p(jnp.exp(-jnp.abs(z)))
    rate = rate_s[...]
    p128[...] = jnp.zeros_like(p128)
    p128[0:heads, :] = -steps_t * rate * LOG2E
    upper = jnp.where(iota((tok, tok), 0) <= iota((tok, tok), 1), 1.0, 0.0).astype(BF16)
    lower = jnp.where(iota((tok, tok), 0) >= iota((tok, tok), 1), 1.0, 0.0).astype(BF16)
    parts = split3(p128[...])
    run_rows = nn(parts[0], upper) + nn(parts[1], upper) + nn(parts[2], upper)
    run_t[...] = run_rows
    run_col = split3(run_rows.T)
    p128[0:heads, :] = steps_t
    steps_col = p128[...].T
    steps_parts = split3(steps_col)

    def onehot(quad):
        return jnp.where(
            iota((LANES, WIDE), 0) == iota((LANES, WIDE), 1) // width + quad * (WIDE // width), 1.0, 0.0
        ).astype(BF16)

    def onehot_t(quad):
        return jnp.where(
            iota((WIDE, LANES), 1) == iota((WIDE, LANES), 0) // width + quad * (WIDE // width), 1.0, 0.0
        ).astype(BF16)

    @pl.loop(0, quads)
    def _(q):
        at = pl.ds(pl.multiple_of(q * WIDE, WIDE), WIDE)
        pick = onehot(q)
        run = nn(run_col[0], pick) + nn(run_col[1], pick) + nn(run_col[2], pick)
        run_s[:, at] = run
        fade = jnp.exp2(run[tok - 1 : tok])
        f_s[2 * q] = jnp.broadcast_to(fade[:, :LANES], (8, LANES))
        f_s[2 * q + 1] = jnp.broadcast_to(fade[:, LANES:], (8, LANES))

    @pl.when(has_prev)
    def _():
        halo_copy.wait_recv()
        ext[0:8] = halo_in[8:16].astype(F32)

    @pl.when(jnp.logical_not(has_prev))
    def _():
        ext[0:8] = jnp.zeros((8, chan), F32)

    def front(q):
        at = pl.ds(pl.multiple_of(q * WIDE, WIDE), WIDE)
        ext[8 : tok + 8, at] = xin[:, at].astype(F32)
        value = jnp.broadcast_to(conv_b[:, at], (tok, WIDE))
        for k in range(4):
            value = value + conv_w[k : k + 1, at] * ext[5 + k : 5 + k + tok, at]
        gate = 1.0 / (1.0 + jnp.exp(-value))
        x_s[:, at] = value * gate
        ds_s[:, at] = gate * (1.0 + value * (1.0 - gate))

    front(quads)
    writes = x_s[:, inner : inner + LANES]
    reads = x_s[:, inner + LANES :]
    b2 = split2(writes)
    c2 = split2(reads)
    ct2 = split2(reads.T)

    @pl.loop(0, quads)
    def _(q):
        at = pl.ds(pl.multiple_of(q * WIDE, WIDE), WIDE)
        w = split2(jnp.exp2(run_s[:, at]) * cot[:, at].astype(F32))
        g = both(nn, ct2, w)
        gt[2 * q] = g[:, :LANES]
        gt[2 * q + 1] = g[:, LANES:]

    def chunk(p):
        return pltpu.make_async_remote_copy(
            src_ref=gt.at[p], dst_ref=et.at[p],
            send_sem=send_sem.at[p], recv_sem=recv_sem.at[p],
            device_id=to(idx - 1), device_id_type=MESH,
        )

    def serve(p):
        @pl.when(has_next)
        def _():
            chunk(p).wait_recv()
            gt[p] = gt[p] + f_s[p][0:1] * et[p]

        @pl.when(jnp.logical_not(has_next))
        def _():
            et[p] = jnp.zeros((LANES, LANES), F32)

        @pl.when(has_prev)
        def _():
            chunk(p).start()

    slot = jnp.minimum((n - 1 - idx) * 4 // 5, quads)

    gram[...] = both(nt, b2, c2)
    dgram[...] = jnp.zeros_like(dgram)
    acc_c[...] = jnp.zeros_like(acc_c)
    acc_b[...] = jnp.zeros_like(acc_b)
    q_acc[...] = jnp.zeros_like(q_acc)
    r_acc[...] = jnp.zeros_like(r_acc)
    last_acc[...] = jnp.zeros_like(last_acc)
    skip_acc[...] = jnp.zeros_like(skip_acc)
    dpos[...] = jnp.zeros_like(dpos)

    low = iota((tok, LANES), 1) < width
    mask = iota((tok, tok), 0) <= iota((tok, tok), 1)

    def pair(p):
        at = pl.ds(pl.multiple_of(p * LANES, LANES), LANES)
        dy = cot[:, at]
        dy_f = dy.astype(F32)
        xs = x_s[:, at] * steps_s[:, at]
        run = run_s[:, at]
        turned = pltpu.roll(run, width, 1)
        twice = jnp.concatenate([dy, dy], axis=1)
        total = jnp.zeros((tok, LANES), F32)
        for half in range(2):
            mine = low if half == 0 else jnp.logical_not(low)
            x_hi, x_lo = split2(jnp.where(mine, xs, 0.0))
            dm = nt(jnp.concatenate([x_hi, x_lo], axis=1), twice)
            own = jnp.where(mine, run, turned)
            own = jnp.concatenate([own, own], axis=1)
            gap = run_t[pl.ds(2 * p + half, 1), :] - own
            fade = jnp.exp2(jnp.where(mask, gap, -jnp.inf))
            ldm = fade * dm
            dgram[...] += ldm
            m = fade * gram[...]
            dpos[pl.ds(2 * p + half, 1), :] = jnp.sum(m * dm, axis=0, keepdims=True)
            m_hi, m_lo = split2(m)
            dy_m = jnp.where(mine, dy_f, 0.0).astype(BF16)
            total = total + nn(m_hi, dy_m) + nn(m_lo, dy_m)
        dxs_s[:, at] = total

    @pl.loop(0, quads)
    def _(q):
        at = pl.ds(pl.multiple_of(q * WIDE, WIDE), WIDE)

        @pl.when(q == slot)
        def _():
            @pl.loop(0, pairs)
            def _(p):
                serve(p)

        front(q)
        pick = onehot(q)
        steps_s[:, at] = nn(steps_parts[0], pick) + nn(steps_parts[1], pick) + nn(steps_parts[2], pick)
        dy = cot[:, at].astype(F32)
        w = jnp.exp2(run_s[:, at]) * dy
        st = state[at, :].T
        hi, lo = split2(st)
        st_hi[:, at] = hi
        st_lo[:, at] = lo
        acc_c[...] += both(nt, split2(w), (hi, lo))
        zy = split2(both(nn, c2, (hi, lo)) * w)
        pick = onehot_t(q)
        r_acc[...] += nn(zy[0], pick) + nn(zy[1], pick)
        sk = split2(jnp.broadcast_to(jnp.sum(dy * x_s[:, at], axis=0, keepdims=True), (8, WIDE)))
        skip_acc[...] += nn(sk[0], pick) + nn(sk[1], pick)

        @pl.loop(0, 2)
        def _(j):
            pair(2 * q + j)

    @pl.loop(0, quads)
    def _(q):
        at = pl.ds(pl.multiple_of(q * WIDE, WIDE), WIDE)

        @pl.when(slot == quads)
        def _():
            serve(2 * q)
            serve(2 * q + 1)

        e = jnp.concatenate([et[2 * q], et[2 * q + 1]], axis=1)
        e2 = split2(e)
        run = run_s[:, at]
        remain = jnp.exp2(run[tok - 1 : tok] - run)
        rv = remain * both(nn, b2, e2)
        steps = steps_s[:, at]
        x = x_s[:, at]
        dxs = rv + dxs_s[:, at]
        xs = x * steps
        pick = onehot_t(q)
        part = split2(x * dxs)
        q_acc[...] += nn(part[0], pick) + nn(part[1], pick)
        st = st_hi[:, at].astype(F32) + st_lo[:, at].astype(F32)
        fade = jnp.exp2(run[tok - 1 : tok])
        end = jnp.sum(xs * rv, axis=0, keepdims=True) + fade * jnp.sum(e * st, axis=0, keepdims=True)
        end = split3(jnp.broadcast_to(end, (8, WIDE)))
        last_acc[...] += nn(end[0], pick) + nn(end[1], pick) + nn(end[2], pick)
        acc_b[...] += both(nt, split2(xs * remain), e2)
        lane = iota((1, WIDE), 1) // width
        gain = jnp.zeros((1, WIDE), F32)
        for j in range(WIDE // width):
            gain = jnp.where(lane == j, skip[q * (WIDE // width) + j], gain)
        dx = dxs * steps + gain * cot[:, at].astype(F32)
        dconv[0:tok, at] = dx * ds_s[:, at]

    dg = split2(dgram[...])
    dgt = split2(dgram[...].T)
    tail = pl.ds(inner, LANES)
    dconv[0:tok, tail] = (acc_b[...] + both(nn, dg, c2)) * ds_s[:, tail]
    tail = pl.ds(inner + LANES, LANES)
    dconv[0:tok, tail] = (acc_c[...] + both(nn, dgt, b2)) * ds_s[:, tail]

    back = pltpu.make_async_remote_copy(
        src_ref=dconv.at[pl.ds(0, 8)], dst_ref=dconv.at[pl.ds(tok, 8)],
        send_sem=back_sem.at[0], recv_sem=back_sem.at[1],
        device_id=to(idx - 1), device_id_type=MESH,
    )

    @pl.when(has_prev)
    def _():
        back.start()

    @pl.when(jnp.logical_not(has_next))
    def _():
        dconv[tok : tok + 8] = jnp.zeros((8, chan), F32)

    drun = r_acc[...] - steps_col * q_acc[...]
    drun = drun + jnp.where(iota((tok, LANES), 0) == tok - 1, last_acc[0:1, :], 0.0)
    dp = split3(drun.T + dpos[...])
    ddecay = (nn(dp[0], lower) + nn(dp[1], lower) + nn(dp[2], lower))[0:heads]
    dsteps = q_acc[...].T[0:heads] - ddecay * rate
    sg = dsteps / (1.0 + jnp.exp(-z))
    step_g[...] = sg
    p128[0:heads, :] = sg
    bf_buf[0, 5:6, 0:LANES] = jnp.sum(p128[...].T, axis=0, keepdims=True)
    p128[0:heads, :] = -ddecay * steps_t * rate
    bf_buf[0, 5:6, LANES : 2 * LANES] = jnp.sum(p128[...].T, axis=0, keepdims=True)
    bf_buf[0, 5:6, 2 * LANES : 3 * LANES] = skip_acc[0:1]
    bf_buf[0, 5:6, 3 * LANES :] = jnp.zeros((1, chan - 3 * LANES), F32)
    bf_buf[0, 6:8, :] = jnp.zeros((2, chan), F32)

    @pl.loop(0, chan // LANES)
    def _(q):
        at = pl.ds(pl.multiple_of(q * LANES, LANES), LANES)
        d = dconv[0:tok, at]
        for k in range(4):
            bf_buf[0, k : k + 1, at] = jnp.sum(d * ext[5 + k : 5 + k + tok, at], axis=0, keepdims=True)
        bf_buf[0, 4:5, at] = jnp.sum(d, axis=0, keepdims=True)

    def swap(k):
        return pltpu.make_async_remote_copy(
            src_ref=bf_buf.at[k], dst_ref=bf_in.at[k],
            send_sem=sum_sem.at[k], recv_sem=sum_sem.at[rounds + k],
            device_id=to(partner(k)), device_id_type=MESH,
        )

    swap(0).start()

    @pl.when(has_next)
    def _():
        back.wait_recv()

    @pl.loop(0, chan // LANES)
    def _(q):
        at = pl.ds(pl.multiple_of(q * LANES, LANES), LANES)
        value = conv_w[3:4, at] * dconv[0:tok, at]
        for k in range(3):
            value = value + conv_w[k : k + 1, at] * dconv[3 - k : 3 - k + tok, at]
        ig[:, at] = value

    for k in range(rounds):
        swap(k).wait_recv()
        bf_buf[k + 1] = bf_buf[k] + bf_in[k]
        if k + 1 < rounds:
            swap(k + 1).start()
    sums_out[...] = bf_buf[rounds]

    for k in range(rounds):
        swap(k).wait_send()

    @pl.when(has_next)
    def _():
        halo_copy.wait_send()

    @pl.when(has_prev)
    def _():
        back.wait_send()

        @pl.loop(0, pairs)
        def _(p):
            chunk(p).wait_send()


def finish(sums, sg, made, ig, kg, off, step_g, bias_g, decay_g, skip_g, held, load_sem, store_sem):
    pieces = load_sem.shape[0]
    rows = held.shape[0] // pieces

    def load(k):
        at = pl.ds(k * rows, rows)
        return pltpu.make_async_copy(made.at[at], held.at[at], load_sem.at[k])

    def store(k):
        at = pl.ds(k * rows, rows)
        return pltpu.make_async_copy(held.at[at], ig.at[at], store_sem.at[k])

    for k in range(pieces):
        load(k).start()
    kg[...] = sums[0:4]
    off[...] = sums[4:5].reshape(off.shape)
    step_g[...] = sg[...]
    for j, ref in enumerate((bias_g, decay_g, skip_g)):
        row = sums[5:6, j * LANES : (j + 1) * LANES]
        ref[...] = row.reshape(LANES)[: ref.shape[0]]
    for k in range(pieces):
        load(k).wait()
        store(k).start()
    for k in range(pieces):
        store(k).wait()


def per_device(
    mixed_input, step_raw, conv_weight, conv_bias, step_bias, decay_log, skip_gain, result_cotangent, entry_state
):
    tok, chan = mixed_input.shape
    _, heads, width, span = entry_state.shape
    inner = heads * width
    n = lax.axis_size("seq")
    rounds = n.bit_length() - 1
    pairs = inner // LANES
    vmem = pl.BlockSpec(memory_space=pltpu.VMEM)
    smem = pl.BlockSpec(memory_space=pltpu.SMEM)
    scr = lambda *shape: pltpu.VMEM(shape, F32)
    outs = pl.pallas_call(
        functools.partial(body, n, heads, width),
        out_shape=(
            jax.ShapeDtypeStruct((tok, chan), F32),
            jax.ShapeDtypeStruct((heads, tok), F32),
            jax.ShapeDtypeStruct((8, chan), F32),
        ),
        in_specs=[vmem] * 4 + [smem] * 3 + [vmem] * 2,
        out_specs=(vmem,) * 3,
        scratch_shapes=[
            scr(tok + 8, chan),
            scr(tok, chan),
            scr(tok, chan),
            scr(tok, inner),
            scr(tok, inner),
            scr(LANES, tok),
            scr(LANES, tok),
            scr(tok, inner),
            pltpu.VMEM((span, inner), BF16),
            pltpu.VMEM((span, inner), BF16),
            scr(pairs, span, LANES),
            scr(pairs, span, LANES),
            scr(pairs, 8, LANES),
            scr(tok, tok),
            scr(tok, tok),
            scr(LANES, tok),
            scr(tok, LANES),
            scr(tok, LANES),
            scr(tok, LANES),
            scr(tok, LANES),
            scr(8, LANES),
            scr(8, LANES),
            scr(tok + 8, chan),
            scr(1, chan),
            scr(heads, tok),
            scr(heads, tok),
            pltpu.VMEM((16, chan), BF16),
            scr(rounds + 1, 8, chan),
            scr(rounds, 8, chan),
            pltpu.SemaphoreType.DMA((pairs,)),
            pltpu.SemaphoreType.DMA((pairs,)),
            pltpu.SemaphoreType.DMA((2,)),
            pltpu.SemaphoreType.DMA((2,)),
            pltpu.SemaphoreType.DMA((2 * rounds,)),
        ],
        compiler_params=pltpu.CompilerParams(
            collective_id=0, has_side_effects=True, vmem_limit_bytes=60 * 1024 * 1024
        ),
    )(
        mixed_input, step_raw, conv_weight, conv_bias, step_bias, decay_log, skip_gain,
        result_cotangent, entry_state.reshape(inner, span),
    )
    made, sg, sums = outs
    hbm = pl.BlockSpec(memory_space=pl.ANY)
    ig, kg, off, step_g, bias_g, decay_g, skip_g = pl.pallas_call(
        finish,
        out_shape=(
            jax.ShapeDtypeStruct((tok, chan), F32),
            jax.ShapeDtypeStruct((4, chan), F32),
            jax.ShapeDtypeStruct((chan,), F32),
            jax.ShapeDtypeStruct((heads, tok), F32),
            jax.ShapeDtypeStruct((heads,), F32),
            jax.ShapeDtypeStruct((heads,), F32),
            jax.ShapeDtypeStruct((heads,), F32),
        ),
        in_specs=[vmem, vmem, hbm],
        out_specs=(hbm,) + (vmem,) * 6,
        scratch_shapes=[scr(tok, chan), pltpu.SemaphoreType.DMA((8,)), pltpu.SemaphoreType.DMA((8,))],
        compiler_params=pltpu.CompilerParams(vmem_limit_bytes=60 * 1024 * 1024),
    )(sums, sg, made)
    return ig, step_g, kg, off, bias_g, decay_g, skip_g


def solution(mesh):
    rows = ("groups", "seq")
    return jax.shard_map(
        per_device,
        mesh=mesh,
        in_specs=(
            P(rows, None), P(None, rows), P(), P(), P(), P(), P(), P(rows, None), P(rows, None, None, None),
        ),
        out_specs=(P(rows, None), P(None, rows), P("groups", None), P("groups"), P("groups"), P("groups"), P("groups")),
        check_vma=False,
    )
```
